32 devices in a mesh: dp: 4 (over y, core), tp: 8 (over z, x).
Axes of the slice: x: 2, y: 2, z: 4, core: 2. Of those that a mesh axis runs over, the one named last changes fastest.
Arguments:
- tokens: bfloat16 [2560, 6144], P(('dp', 'tp')), parts along dimension 0, may hold values from -6 to 6
- ln_gain: float32 [6144], replicated, may hold values from 0.25 to 1.75
- ln_bias: float32 [6144], replicated, may hold values from -1.75 to 1.75
- w_qkv: bfloat16 [6144, 3, 6144], P(None, None, 'tp'), may hold values from -0.45927933 to 0.45927933
- b_qkv: float32 [3, 6144], P(None, 'tp'), may hold values from -3 to 3
- w_out: bfloat16 [6144, 6144], P('tp'), may hold values from -0.078125 to 0.078125
- b_out: float32 [6144], replicated, may hold values from -1.25 to 1.25
- kv_cache: bfloat16 [2, 28, 128, 6144], P(None, 'dp', None, 'tp'), parts along dimension 1, may hold values from -6 to 6
- page_table: int32 [4, 5], P('dp'), parts along dimension 0, may hold values from 0 to 6, as said below
- lengths: int32 [4], P('dp'), parts along dimension 0, may hold values from 321 to 640
Outputs:
- attn_out: bfloat16 [2560, 6144], P(('dp', 'tp')), parts along dimension 0
- kv_cache_out: bfloat16 [2, 28, 128, 6144], P(None, 'dp', None, 'tp'), parts along dimension 1
The draws below stay inside these ranges and needn't reach their ends.
There are 4 independent parts, one for each index of `dp`. The reference program is written for one: setup_inputs(seed, part) draws one part's arguments, and reference() takes and returns one part's arrays. A program takes and returns all parts, laid end to end along the dimension named above; an argument that names none is the same for every part. Nothing has to cross between parts.
Inputs may be any that keep to these rules, and one draw needn't show every extreme that they name: `page_table`: no slot is named twice within a part.
All inputs are finite; a program needn't handle non-finite values.
Results may differ from the reference program's by a relative error of at most 0.015.
The reference program's roundings to bfloat16 on the way (of `normed`, `projected`, `weights` and `attended`) count: a program that leaves them out, or rounds other values in their place, can miss the bound.
Values may be sent and summed in bfloat16 or wider, within the bound.
A program may use at most 128 MiB of HBM per device.

```python
import math
import jax
import jax.numpy as jnp
from jax import lax

D = 6144
HEADS = 48
HD = 128
SEQS = 1
PAGE = 128
FEAT = 6144
TOKENS = 640
LEN = 640
PAGES = 5
SLOTS = 7


def draw_w_qkv(key, part):
    normal_part = jnp.clip(jax.random.normal(jax.random.fold_in(key, 5), (D, 3, FEAT), jnp.float32), -6.0, 6.0) * (1.0 / math.sqrt(D))
    return normal_part.astype(jnp.bfloat16)


def draw_page_table(key, part):
    shuffled = jax.random.permutation(jax.random.fold_in(key, 11), SLOTS)
    return shuffled[:SEQS * PAGES].reshape(SEQS, PAGES).astype(jnp.int32)


def block_levels(rng, shape, pieces, low, top_value):
    level = 1.0
    for position, blocks in pieces:
        heights = jax.random.uniform(jax.random.fold_in(jax.random.fold_in(rng, 6), position), (blocks,), jnp.float32, low / len(pieces), top_value / len(pieces))
        level = level * jnp.repeat(jnp.exp(heights), shape[position] // blocks).reshape((-1,) + (1,) * (len(shape) - 1 - position))
    return level


def bell_draw(rng, dims, scale, most, shards=(), kind=jnp.bfloat16):
    drawn = jax.random.normal(rng, dims, jnp.float32) * scale
    if len(shards) > 0:
        drawn = block_levels(rng, dims, shards, -0.22, 0.18) * drawn
    return jnp.clip(drawn, min=-most, max=most).astype(kind)


def setup_inputs(seed: int = 0, part: int = 0) -> dict:
    arg_keys = jax.random.split(jax.random.key(seed), 11)
    own_keys = jax.random.split(jax.random.fold_in(arg_keys[10], part), 11)
    tokens = bell_draw(own_keys[0], (TOKENS, D), 1.0, 6.0, ((0, 8),))
    ln_gain = jnp.clip(1.0 + 0.15 * jax.random.normal(arg_keys[1], (D,), jnp.float32), 0.25, 1.75)
    ln_bias = bell_draw(arg_keys[2], (D,), 0.3, 1.75, (), jnp.float32)
    w_qkv = draw_w_qkv(jax.random.fold_in(arg_keys[10], 71), part)
    b_qkv = bell_draw(arg_keys[4], (3, FEAT), 0.5, 3.0, ((1, 8),), jnp.float32)
    w_out = bell_draw(arg_keys[5], (FEAT, D), FEAT ** -0.5, 0.078125, ((0, 8),))
    b_out = bell_draw(arg_keys[6], (D,), 0.2, 1.25, (), jnp.float32)
    kv_cache = bell_draw(own_keys[7], (2, SLOTS, PAGE, FEAT), 1.0, 6.0, ((3, 8),))
    page_table = draw_page_table(jax.random.fold_in(jax.random.fold_in(arg_keys[10], part), 71), part)
    lengths = jax.random.randint(own_keys[9], (SEQS,), LEN // 2 + 1, LEN + 1).astype(jnp.int32)
    return {"tokens": tokens, "ln_gain": ln_gain, "ln_bias": ln_bias, "w_qkv": w_qkv, "b_qkv": b_qkv, "w_out": w_out, "b_out": b_out, "kv_cache": kv_cache, "page_table": page_table, "lengths": lengths}


norm_eps = 1e-05

def layer_norm(token_rows, gain_row, shift_row):
    floats = token_rows.astype(jnp.float32)
    center = lax.optimization_barrier(jnp.mean(floats, axis=-1, keepdims=True))
    spread = lax.optimization_barrier(jnp.mean(jnp.square(floats - center), axis=-1, keepdims=True))
    return ((floats - center) * lax.rsqrt(spread + norm_eps) * gain_row + shift_row).astype(jnp.bfloat16)

def attend(queries, keys, values, lengths):
    seq_count, seq_len, head_count, head_dim = queries.shape
    block_len = math.gcd(seq_len, 512)
    score_scale = 1.0 / math.sqrt(head_dim)
    key_pos = jnp.arange(seq_len, dtype=jnp.int32)

    def one_sequence(inputs):
        seq_query, seq_key, seq_value, length = inputs
        blocks = seq_query.reshape(seq_len // block_len, block_len, head_count, head_dim)

        def one_block(block_pair):
            block_query, block_index = block_pair
            scores = jnp.einsum('qhe,khe->hqk', block_query.astype(jnp.float32), seq_key.astype(jnp.float32)) * score_scale
            query_pos = block_index * block_len + jnp.arange(block_len, dtype=jnp.int32)
            allowed = (key_pos[None, :] <= query_pos[:, None]) & (key_pos[None, :] < length)
            scores = jnp.where(allowed[None], scores, -1e+30)
            row_max = lax.optimization_barrier(jnp.max(scores, axis=-1, keepdims=True))
            raised = jnp.exp(scores - row_max)
            weights = (raised / lax.optimization_barrier(jnp.sum(raised, axis=-1, keepdims=True))).astype(jnp.bfloat16)
            return jnp.einsum('hqk,khe->qhe', weights.astype(jnp.float32), seq_value.astype(jnp.float32)).astype(jnp.bfloat16)
        results = lax.map(one_block, (blocks, jnp.arange(seq_len // block_len, dtype=jnp.int32)))
        return results.reshape(seq_len, head_count, head_dim)
    return lax.map(one_sequence, (queries, keys, values, lengths.astype(jnp.int32)))

def write_cache(kv_cache, key_value, page_table, lengths):
    seq_count, page_count = page_table.shape
    page_len = kv_cache.shape[2]
    feat_here = kv_cache.shape[3]
    fresh_pages = jnp.moveaxis(key_value, 1, 0).reshape(2, seq_count * page_count, page_len, feat_here)
    slot_ids = page_table.reshape(-1).astype(jnp.int32)
    positions = jnp.arange(page_count, dtype=jnp.int32)[:, None] * page_len + jnp.arange(page_len, dtype=jnp.int32)[None, :]
    written = (positions[None] < lengths.astype(jnp.int32)[:, None, None]).reshape(seq_count * page_count, page_len)
    current = kv_cache[:, slot_ids]
    new_pages = jnp.where(written[None, :, :, None], fresh_pages, current)
    return kv_cache.at[:, slot_ids].set(new_pages)

def reference(tokens, ln_gain, ln_bias, w_qkv, b_qkv, w_out, b_out, kv_cache, page_table, lengths):
    normed = layer_norm(tokens, ln_gain, ln_bias)
    flat = jnp.dot(normed, w_qkv.reshape(D, 3 * FEAT), preferred_element_type=jnp.float32) + b_qkv.reshape(-1)
    projected = flat.astype(jnp.bfloat16).reshape(TOKENS, 3, FEAT)
    queries = projected[:, 0].reshape(SEQS, LEN, HEADS, HD)
    keys = projected[:, 1].reshape(SEQS, LEN, HEADS, HD)
    values = projected[:, 2].reshape(SEQS, LEN, HEADS, HD)
    attended = attend(queries, keys, values, lengths).reshape(TOKENS, FEAT)
    attn_out = (jnp.dot(attended, w_out, preferred_element_type=jnp.float32) + b_out).astype(jnp.bfloat16)
    kv_cache_out = write_cache(kv_cache, projected[:, 1:3], page_table, lengths)
    return (attn_out, kv_cache_out)
```

```python
import functools
import math

import jax
import jax.numpy as jnp
import numpy as np
from jax import lax
from jax.experimental import pallas as pl
from jax.experimental.pallas import tpu as pltpu
from jax.sharding import PartitionSpec as P

HD = 128
CHUNKS = 4
MESH = pl.DeviceIdType.MESH

norm_eps = 1e-05


def layer_norm(token_rows, gain_row, shift_row):
    floats = token_rows.astype(jnp.float32)
    center = jnp.mean(floats, axis=-1, keepdims=True)
    spread = jnp.mean(jnp.square(floats - center), axis=-1, keepdims=True)
    return ((floats - center) * lax.rsqrt(spread + norm_eps) * gain_row + shift_row).astype(
        jnp.bfloat16
    )


def ring_order(mesh):
    n = mesh.shape["tp"]
    line = np.moveaxis(mesh.devices, mesh.axis_names.index("tp"), -1).reshape(-1, n)[0]
    coords = [tuple(getattr(d, "coords", None) or ()) for d in line]
    wide = len({c[0] for c in coords if c})
    if wide < 2 or n % wide or (n // wide) % 2:
        return list(range(n))
    tall = n // wide
    order = [0]
    for z in range(tall):
        xs = range(1, wide) if z % 2 == 0 else range(wide - 1, 0, -1)
        order += [z * wide + x for x in xs]
    order += [z * wide for z in range(tall - 1, 0, -1)]
    return order


def pick(table, index):
    value = jnp.int32(0)
    for k, entry in enumerate(table):
        value = value + jnp.where(index == k, entry, 0)
    return value


def fused(order, x_ref, w_hbm, b_ref, wo_hbm, bo_ref, len_ref, out_ref, kv_hbm,
          xg, w_v, wo_v, proj, att, first, rs,
          ag_send, ag_recv, rs_send, rs_recv, w_sem, wo_sem, kv_sem):
    n = len(order)
    h = n // 2
    rows, model = x_ref.shape
    mid = model // 2
    feat = w_v.shape[2]
    total = proj.shape[1]
    me = lax.axis_index("tp")
    inverse = [order.index(i) for i in range(n)]
    place = pick(inverse, me)

    def at(offset):
        return pick(order, lax.rem(place + offset + n, n))

    peers = (at(1), at(-1))
    for c in range(3):
        pltpu.make_async_copy(w_hbm.at[c], w_v.at[c], w_sem.at[c]).start()

    barrier = pltpu.get_barrier_semaphore()
    for peer in peers:
        pl.semaphore_signal(barrier, inc=1, device_id={"tp": peer}, device_id_type=MESH)
    pl.semaphore_wait(barrier, 2)

    def slot(way, s):
        return n - 1 if s == h else 2 * s - 1 + way

    def gather(way, s, half):
        dst = xg.at[half, pl.ds(slot(way, s) * rows, rows)]
        if s == 1:
            src = x_ref.at[:, pl.ds(half * mid, mid)]
        else:
            src = xg.at[half, pl.ds(slot(way, s - 1) * rows, rows)]
        return pltpu.make_async_remote_copy(
            src_ref=src, dst_ref=dst,
            send_sem=ag_send.at[way, s, half], recv_sem=ag_recv.at[way, s, half],
            device_id={"tp": peers[way]}, device_id_type=MESH)

    gathers = [(way, s, half) for s in range(1, h + 1) for half in range(2) for way in range(2)
               if s < h or way == half]
    for g in gathers:
        if g[1] == 1:
            gather(*g).start()
    wo_copy = pltpu.make_async_copy(wo_hbm, wo_v, wo_sem)
    wo_copy.start()
    for c in range(3):
        pltpu.make_async_copy(w_hbm.at[c], w_v.at[c], w_sem.at[c]).wait()

    tn = math.gcd(feat, 256)

    def project(lhs, owners):
        @pl.loop(0, 3)
        def _(c):
            @pl.loop(0, feat // tn)
            def _(j):
                cols = pl.ds(pl.multiple_of(j * tn, tn), tn)
                acc = jnp.dot(lhs(0), w_v[c, pl.ds(0, mid), cols],
                              preferred_element_type=jnp.float32)
                acc += jnp.dot(lhs(1), w_v[c, pl.ds(mid, mid), cols],
                               preferred_element_type=jnp.float32)
                done = (acc + b_ref[c, :, cols]).astype(jnp.bfloat16)
                for i, owner in enumerate(owners):
                    dst = pl.ds(pl.multiple_of(owner * rows, rows), rows)
                    proj[c, dst, cols] = done[i * rows:(i + 1) * rows]

    project(lambda half: x_ref[:, pl.ds(half * mid, mid)], [me])
    for s in range(1, h + 1):
        for half in range(2):
            for way in range(2):
                if (way, s, half) in gathers:
                    gather(way, s, half).wait_recv()
                    if (way, s + 1, half) in gathers:
                        gather(way, s + 1, half).start()
        if s < h:
            project(lambda half: xg[half, pl.ds((2 * s - 1) * rows, 2 * rows)], [at(-s), at(s)])
        else:
            project(lambda half: xg[half, pl.ds((n - 1) * rows, rows)], [at(h)])
    kv_copy = pltpu.make_async_copy(proj.at[pl.ds(1, 2)], kv_hbm, kv_sem)
    kv_copy.start()

    scale = 1.0 / math.sqrt(HD)
    length = len_ref[0]

    def attend(owners):
        key_pos = lax.broadcasted_iota(jnp.int32, (rows, total), 1)
        row_pos = lax.broadcasted_iota(jnp.int32, (rows, total), 0)

        @pl.loop(0, feat // HD)
        def _(head):
            cols = pl.ds(pl.multiple_of(head * HD, HD), HD)
            key, value = proj[1, :, cols], proj[2, :, cols]
            for i, owner in enumerate(owners):
                query = proj[0, pl.ds(pl.multiple_of(owner * rows, rows), rows), cols]
                scores = lax.dot_general(query, key, (((1,), (1,)), ((), ())),
                                         preferred_element_type=jnp.float32) * scale
                allowed = (key_pos <= row_pos + owner * rows) & (key_pos < length)
                scores = jnp.where(allowed, scores, -1e30)
                raised = jnp.exp(scores - jnp.max(scores, axis=-1, keepdims=True))
                weights = (raised / jnp.sum(raised, axis=-1, keepdims=True)).astype(jnp.bfloat16)
                att[pl.ds(i * rows, rows), cols] = jnp.dot(
                    weights, value, preferred_element_type=jnp.float32).astype(jnp.bfloat16)

    chunk = model // CHUNKS
    to = math.gcd(chunk, 512)

    def scatter(way, d, q):
        cols = pl.ds(q * chunk, chunk)
        src = first.at[:, cols] if d == h else rs.at[way, d, :, cols]
        return pltpu.make_async_remote_copy(
            src_ref=src, dst_ref=rs.at[way, d - 1, :, cols],
            send_sem=rs_send.at[way, d, q], recv_sem=rs_recv.at[way, d, q],
            device_id={"tp": peers[way]}, device_id_type=MESH)

    scatters = [(way, d, q) for d in range(h, 0, -1) for q in range(CHUNKS) for way in range(2)
                if d < h or way == q // (CHUNKS // 2)]

    wo_copy.wait()
    attend([at(h)])
    for q in range(CHUNKS):
        @pl.loop(0, chunk // to)
        def _(j):
            cols = pl.ds(pl.multiple_of(q * chunk + j * to, to), to)
            first[:, cols] = jnp.dot(att[pl.ds(0, rows), :], wo_v[:, cols],
                                     preferred_element_type=jnp.float32).astype(jnp.bfloat16)
        for way in range(2):
            if (way, h, q) in scatters:
                scatter(way, h, q).start()

    for d in range(h - 1, 0, -1):
        attend([at(d), at(-d)])
        half = CHUNKS // 2
        for q in ([0, half] + [c for c in range(CHUNKS) if c not in (0, half)]):
            have = [(way, d + 1, q) in scatters for way in range(2)]
            for way in range(2):
                if have[way]:
                    scatter(way, d + 1, q).wait_recv()

            @pl.loop(0, chunk // to)
            def _(j):
                cols = pl.ds(pl.multiple_of(q * chunk + j * to, to), to)
                part = jnp.dot(att[...], wo_v[:, cols], preferred_element_type=jnp.float32)
                for way in range(2):
                    mine = part[way * rows:(way + 1) * rows]
                    if have[way]:
                        mine = mine + rs[way, d, :, cols].astype(jnp.float32)
                    rs[way, d, :, cols] = mine.astype(jnp.bfloat16)
            for way in range(2):
                scatter(way, d, q).start()

    attend([me])
    half = CHUNKS // 2
    for q in ([0, half] + [c for c in range(CHUNKS) if c not in (0, half)]):
        for way in range(2):
            scatter(way, 1, q).wait_recv()

        @pl.loop(0, chunk // to)
        def _(j):
            cols = pl.ds(pl.multiple_of(q * chunk + j * to, to), to)
            part = jnp.dot(att[pl.ds(0, rows), :], wo_v[:, cols],
                           preferred_element_type=jnp.float32)
            part += rs[0, 0, :, cols].astype(jnp.float32) + rs[1, 0, :, cols].astype(jnp.float32)
            out_ref[:, cols] = (part + bo_ref[:, cols]).astype(jnp.bfloat16)

    for g in gathers:
        gather(*g).wait_send()
    for g in scatters:
        scatter(*g).wait_send()
    kv_copy.wait()


def fill_page(pages_ref, length_ref, cache_ref, fresh_ref, out_ref):
    page = pages_ref[pl.program_id(0)]
    page_len = out_ref.shape[2]
    left = jnp.where(page >= 0, length_ref[0] - page * page_len, 0)
    pos = lax.broadcasted_iota(jnp.int32, (2, 1, page_len, 1), 2)
    out_ref[...] = jnp.where(pos < left, fresh_ref[...], cache_ref[...])


def write_cache(kv_cache, fresh, page_table, lengths):
    two, slots, page_len, feat = kv_cache.shape
    page_count = page_table.shape[1]
    hits = page_table[0][None, :] == jnp.arange(slots, dtype=jnp.int32)[:, None]
    pages = jnp.max(jnp.where(hits, jnp.arange(page_count, dtype=jnp.int32)[None], -1), axis=1)
    block = (2, 1, page_len, feat)
    return pl.pallas_call(
        fill_page,
        grid_spec=pltpu.PrefetchScalarGridSpec(
            num_scalar_prefetch=2,
            grid=(slots,),
            in_specs=[
                pl.BlockSpec(block, lambda s, pages, length: (0, s, 0, 0)),
                pl.BlockSpec(block, lambda s, pages, length: (0, jnp.maximum(pages[s], 0), 0, 0)),
            ],
            out_specs=pl.BlockSpec(block, lambda s, pages, length: (0, s, 0, 0)),
        ),
        out_shape=jax.ShapeDtypeStruct(kv_cache.shape, kv_cache.dtype),
        name="fill_pages",
    )(pages, lengths, kv_cache, fresh)


def body(order, tokens, ln_gain, ln_bias, w_qkv, b_qkv, w_out, b_out, kv_cache, page_table,
         lengths):
    n = len(order)
    h = n // 2
    rows, model = tokens.shape
    feat = w_qkv.shape[2]
    total = rows * n
    normed = layer_norm(tokens, ln_gain, ln_bias)
    vmem = pl.BlockSpec(memory_space=pltpu.VMEM)
    anywhere = pl.BlockSpec(memory_space=pl.ANY)
    bf16 = jnp.bfloat16
    attn_out, fresh = pl.pallas_call(
        functools.partial(fused, order),
        out_shape=(
            jax.ShapeDtypeStruct((rows, model), bf16),
            jax.ShapeDtypeStruct((2, total, feat), bf16),
        ),
        in_specs=[vmem, anywhere, vmem, anywhere, vmem, pl.BlockSpec(memory_space=pltpu.SMEM)],
        out_specs=(vmem, anywhere),
        scratch_shapes=[
            pltpu.VMEM((2, total, model // 2), bf16),
            pltpu.VMEM((3, model, feat), bf16),
            pltpu.VMEM((feat, model), bf16),
            pltpu.VMEM((3, total, feat), bf16),
            pltpu.VMEM((2 * rows, feat), bf16),
            pltpu.VMEM((rows, model), bf16),
            pltpu.VMEM((2, h, rows, model), bf16),
            pltpu.SemaphoreType.DMA((2, h + 1, 2)),
            pltpu.SemaphoreType.DMA((2, h + 1, 2)),
            pltpu.SemaphoreType.DMA((2, h + 1, CHUNKS)),
            pltpu.SemaphoreType.DMA((2, h + 1, CHUNKS)),
            pltpu.SemaphoreType.DMA((3,)),
            pltpu.SemaphoreType.DMA,
            pltpu.SemaphoreType.DMA,
        ],
        compiler_params=pltpu.CompilerParams(
            collective_id=0, has_side_effects=True, vmem_limit_bytes=67_043_328
        ),
        name="attention_sublayer",
    )(normed, jnp.transpose(w_qkv, (1, 0, 2)), b_qkv[:, None, :], w_out, b_out[None, :], lengths)
    page_len = kv_cache.shape[2]
    fresh = fresh.reshape(2, total // page_len, page_len, feat)
    return attn_out, write_cache(kv_cache, fresh, page_table, lengths)


def solution(mesh):
    placed = (
        P(("dp", "tp"), None),
        P(),
        P(),
        P(None, None, "tp"),
        P(None, "tp"),
        P("tp", None),
        P(),
        P(None, "dp", None, "tp"),
        P("dp", None),
        P("dp"),
    )
    return jax.shard_map(
        functools.partial(body, ring_order(mesh)),
        mesh=mesh,
        in_specs=placed,
        out_specs=(P(("dp", "tp"), None), P(None, "dp", None, "tp")),
        check_vma=False,
    )
```

```python
import functools
import math

import jax
import jax.numpy as jnp
import numpy as np
from jax import lax
from jax.experimental import pallas as pl
from jax.experimental.pallas import tpu as pltpu
from jax.sharding import PartitionSpec as P

HD = 128
CHUNKS = 4
PIECES = 4
MESH = pl.DeviceIdType.MESH

norm_eps = 1e-05


def ring_order(mesh):
    n = mesh.shape["tp"]
    line = np.moveaxis(mesh.devices, mesh.axis_names.index("tp"), -1).reshape(-1, n)[0]
    coords = [tuple(getattr(d, "coords", None) or ()) for d in line]
    wide = len({c[0] for c in coords if c})
    if wide < 2 or n % wide or (n // wide) % 2:
        return list(range(n))
    tall = n // wide
    order = [0]
    for z in range(tall):
        xs = range(1, wide) if z % 2 == 0 else range(wide - 1, 0, -1)
        order += [z * wide + x for x in xs]
    order += [z * wide for z in range(tall - 1, 0, -1)]
    return order


def pick(table, index):
    value = jnp.int32(0)
    for k, entry in enumerate(table):
        value = value + jnp.where(index == k, entry, 0)
    return value


def fused(order, x_hbm, gain_ref, shift_ref, w_hbm, b_ref, wo_hbm, bo_ref, cache_hbm, table_ref,
          len_ref, out_ref, kv_hbm,
          xg, w_v, wo_v, proj, att, first, rs, held, bias,
          ag_send, ag_recv, tail_send, tail_recv, rs_send, rs_recv,
          x_sem, w_sem, wo_sem, in_sem, kv_sem):
    n = len(order)
    h = n // 2
    rows, model = x_hbm.shape
    mid = model // 2
    feat = w_v.shape[2]
    total = proj.shape[1]
    me = lax.axis_index("tp")
    inverse = [order.index(i) for i in range(n)]
    place = pick(inverse, me)

    def at(offset):
        return pick(order, lax.rem(place + offset + n, n))

    peers = (at(1), at(-1))
    x_copy = pltpu.make_async_copy(x_hbm, first, x_sem)
    x_copy.start()
    barrier = pltpu.get_barrier_semaphore()
    for peer in peers:
        pl.semaphore_signal(barrier, inc=1, device_id={"tp": peer}, device_id_type=MESH)
    x_copy.wait()
    for c in range(3):
        pltpu.make_async_copy(w_hbm.at[c], w_v.at[c], w_sem.at[c]).start()
    wo_copy = pltpu.make_async_copy(wo_hbm, wo_v, wo_sem)
    wo_copy.start()

    for c in range(3):
        bias[c] = b_ref[pl.ds(c, 1), :]
    group = math.gcd(rows, 16)

    @pl.loop(0, rows // group)
    def _(i):
        part = pl.ds(pl.multiple_of(i * group, group), group)
        floats = first[part, :].astype(jnp.float32)
        center = jnp.mean(floats, axis=-1, keepdims=True)
        spread = jnp.mean(jnp.square(floats - center), axis=-1, keepdims=True)
        normed = ((floats - center) * lax.rsqrt(spread + norm_eps) * gain_ref[...]
                  + shift_ref[...]).astype(jnp.bfloat16)
        xg[0, part, :] = normed[:, :mid]
        xg[1, part, :] = normed[:, mid:]

    pl.semaphore_wait(barrier, 2)

    def slot(way, s):
        return 0 if s == 0 else n - 1 if s == h else 2 * s - 1 + way

    def gather(way, s, half):
        return pltpu.make_async_remote_copy(
            src_ref=xg.at[half, pl.ds(slot(way, s - 1) * rows, rows)],
            dst_ref=xg.at[half, pl.ds(slot(way, s) * rows, rows)],
            send_sem=ag_send.at[way, s, half], recv_sem=ag_recv.at[way, s, half],
            device_id={"tp": peers[way]}, device_id_type=MESH)

    piece = mid // PIECES

    def tail(way, e):
        cols = pl.ds(e * piece, piece)
        return pltpu.make_async_remote_copy(
            src_ref=xg.at[way, pl.ds(slot(way, h - 1) * rows, rows), cols],
            dst_ref=xg.at[way, pl.ds((n - 1) * rows, rows), cols],
            send_sem=tail_send.at[way, e], recv_sem=tail_recv.at[way, e],
            device_id={"tp": peers[way]}, device_id_type=MESH)

    gathers = [(way, s, k if way == 0 else 1 - k)
               for s in range(1, h) for k in range(2) for way in range(2)]
    for g in gathers:
        if g[1] == 1:
            gather(*g).start()
    for c in range(3):
        pltpu.make_async_copy(w_hbm.at[c], w_v.at[c], w_sem.at[c]).wait()

    tn = math.gcd(feat, 256)

    def project(lhs, owners):
        @pl.loop(0, 3)
        def _(c):
            @pl.loop(0, feat // tn)
            def _(j):
                cols = pl.ds(pl.multiple_of(j * tn, tn), tn)
                acc = jnp.dot(lhs(0), w_v[c, pl.ds(0, mid), cols],
                              preferred_element_type=jnp.float32)
                acc += jnp.dot(lhs(1), w_v[c, pl.ds(mid, mid), cols],
                               preferred_element_type=jnp.float32)
                done = (acc + bias[c, :, cols]).astype(jnp.bfloat16)
                for i, owner in enumerate(owners):
                    dst = pl.ds(pl.multiple_of(owner * rows, rows), rows)
                    proj[c, dst, cols] = done[i * rows:(i + 1) * rows]

    def project_tail(e):
        far = pl.ds((n - 1) * rows, rows)
        here = pl.ds(e * piece, piece)

        @pl.loop(0, 3)
        def _(c):
            @pl.loop(0, feat // tn)
            def _(j):
                cols = pl.ds(pl.multiple_of(j * tn, tn), tn)
                acc = jnp.dot(xg[0, far, here], w_v[c, here, cols],
                              preferred_element_type=jnp.float32)
                acc += jnp.dot(xg[1, far, here], w_v[c, pl.ds(mid + e * piece, piece), cols],
                               preferred_element_type=jnp.float32)
                if e > 0:
                    acc += held[c, :, cols]
                if e < PIECES - 1:
                    held[c, :, cols] = acc
                else:
                    dst = pl.ds(pl.multiple_of(at(h) * rows, rows), rows)
                    proj[c, dst, cols] = (acc + bias[c, :, cols]).astype(jnp.bfloat16)

    project(lambda half: xg[half, pl.ds(0, rows)], [me])
    for s in range(1, h):
        for g in gathers:
            if g[1] == s:
                way, _, half = g
                gather(*g).wait_recv()
                if s + 1 < h:
                    gather(way, s + 1, half).start()
                elif half == way:
                    for e in range(PIECES):
                        tail(way, e).start()
        project(lambda half: xg[half, pl.ds((2 * s - 1) * rows, 2 * rows)], [at(-s), at(s)])
    for e in range(PIECES):
        for way in range(2):
            tail(way, e).wait_recv()
        project_tail(e)

    slots, page_len = cache_hbm.shape[1:3]

    def page(i, s):
        return w_v.at[i, pl.ds(s * page_len, page_len)]

    def cache_in(i, s):
        return pltpu.make_async_copy(cache_hbm.at[i, s], page(i, s), in_sem.at[i, s])

    def cache_out(i, s):
        return pltpu.make_async_copy(page(i, s), kv_hbm.at[i, s], kv_sem.at[i, s])

    pages = [(i, s) for i in range(2) for s in range(slots)]
    length = len_ref[0]

    def fill_pages():
        for i, s in pages:
            cache_in(i, s).wait()
        pos = lax.broadcasted_iota(jnp.int32, (page_len, feat), 0)

        @pl.loop(0, slots)
        def _(s):
            here = pl.ds(pl.multiple_of(s * page_len, page_len), page_len)
            for i in range(2):
                held_page = w_v[i, here, :]
                for k in range(table_ref.shape[1]):
                    left = jnp.where(table_ref[0, k] == s, length - k * page_len, 0)
                    held_page = jnp.where(
                        pos < left, proj[i + 1, pl.ds(k * page_len, page_len), :], held_page)
                w_v[i, here, :] = held_page

        for i, s in pages:
            cache_out(i, s).start()

    scale = 1.0 / math.sqrt(HD)

    def attend(owners):
        key_pos = lax.broadcasted_iota(jnp.int32, (rows, total), 1)
        row_pos = lax.broadcasted_iota(jnp.int32, (rows, total), 0)

        heads = feat // HD
        per = 1 if len(owners) > 1 else math.gcd(heads, 3)

        @pl.loop(0, heads // per)
        def _(turn):
            for i, b in [(i, b) for i in range(per) for b in range(len(owners))]:
                owner = owners[b]
                cols = pl.ds(pl.multiple_of((turn * per + i) * HD, HD), HD)
                query = proj[0, pl.ds(pl.multiple_of(owner * rows, rows), rows), cols]
                scores = lax.dot_general(query, proj[1, :, cols], (((1,), (1,)), ((), ())),
                                         preferred_element_type=jnp.float32) * scale
                allowed = (key_pos <= row_pos + owner * rows) & (key_pos < length)
                scores = jnp.where(allowed, scores, -1e30)
                raised = jnp.exp(scores - jnp.max(scores, axis=-1, keepdims=True))
                share = 1.0 / jnp.sum(raised, axis=-1, keepdims=True)
                att[pl.ds(b * rows, rows), cols] = jnp.dot(
                    (raised * share).astype(jnp.bfloat16), proj[2, :, cols],
                    preferred_element_type=jnp.float32).astype(jnp.bfloat16)

    chunk = model // CHUNKS
    to = math.gcd(chunk, 512)

    def scatter(way, d, q):
        cols = pl.ds(q * chunk, chunk)
        src = first.at[:, cols] if d == h else rs.at[way, d, :, cols]
        return pltpu.make_async_remote_copy(
            src_ref=src, dst_ref=rs.at[way, d - 1, :, cols],
            send_sem=rs_send.at[way, d, q], recv_sem=rs_recv.at[way, d, q],
            device_id={"tp": peers[way]}, device_id_type=MESH)

    scatters = [(way, d, q) for d in range(h, 0, -1) for q in range(CHUNKS) for way in range(2)
                if d < h or way == q // (CHUNKS // 2)]

    wo_copy.wait()
    attend([at(h)])
    half = CHUNKS // 2
    turns = [0, half] + [c for c in range(CHUNKS) if c not in (0, half)]
    for q in turns:
        @pl.loop(0, chunk // to)
        def _(j):
            cols = pl.ds(pl.multiple_of(q * chunk + j * to, to), to)
            first[:, cols] = jnp.dot(att[pl.ds(0, rows), :], wo_v[:, cols],
                                     preferred_element_type=jnp.float32).astype(jnp.bfloat16)
        for way in range(2):
            if (way, h, q) in scatters:
                scatter(way, h, q).start()

    for i, s in pages:
        cache_in(i, s).start()

    for d in range(h - 1, 0, -1):
        attend([at(d), at(-d)])
        for q in turns:
            have = [(way, d + 1, q) in scatters for way in range(2)]
            for way in range(2):
                if have[way]:
                    scatter(way, d + 1, q).wait_recv()

            @pl.loop(0, chunk // to)
            def _(j):
                cols = pl.ds(pl.multiple_of(q * chunk + j * to, to), to)
                part = jnp.dot(att[...], wo_v[:, cols], preferred_element_type=jnp.float32)
                for way in range(2):
                    mine = part[way * rows:(way + 1) * rows]
                    if have[way]:
                        mine = mine + rs[way, d, :, cols].astype(jnp.float32)
                    rs[way, d, :, cols] = mine.astype(jnp.bfloat16)
            for way in range(2):
                scatter(way, d, q).start()
        if d == h - 1:
            fill_pages()

    attend([me])
    for q in turns:
        for way in range(2):
            scatter(way, 1, q).wait_recv()

        @pl.loop(0, chunk // to)
        def _(j):
            cols = pl.ds(pl.multiple_of(q * chunk + j * to, to), to)
            part = jnp.dot(att[pl.ds(0, rows), :], wo_v[:, cols],
                           preferred_element_type=jnp.float32)
            part += rs[0, 0, :, cols].astype(jnp.float32) + rs[1, 0, :, cols].astype(jnp.float32)
            out_ref[:, cols] = (part + bo_ref[:, cols]).astype(jnp.bfloat16)

    for g in gathers:
        gather(*g).wait_send()
    for e in range(PIECES):
        for way in range(2):
            tail(way, e).wait_send()
    for g in scatters:
        scatter(*g).wait_send()
    for i, s in pages:
        cache_out(i, s).wait()


def body(order, tokens, ln_gain, ln_bias, w_qkv, b_qkv, w_out, b_out, kv_cache, page_table,
         lengths):
    n = len(order)
    h = n // 2
    rows, model = tokens.shape
    feat = w_qkv.shape[2]
    total = rows * n
    vmem = pl.BlockSpec(memory_space=pltpu.VMEM)
    anywhere = pl.BlockSpec(memory_space=pl.ANY)
    bf16 = jnp.bfloat16
    smem = pl.BlockSpec(memory_space=pltpu.SMEM)
    slots = kv_cache.shape[1]
    dma = pltpu.SemaphoreType.DMA
    return pl.pallas_call(
        functools.partial(fused, order),
        out_shape=(
            jax.ShapeDtypeStruct((rows, model), bf16),
            jax.ShapeDtypeStruct(kv_cache.shape, bf16),
        ),
        in_specs=[anywhere, vmem, vmem, anywhere, vmem, anywhere, vmem, anywhere, smem, smem],
        out_specs=(vmem, anywhere),
        scratch_shapes=[
            pltpu.VMEM((2, total, model // 2), bf16),
            pltpu.VMEM((3, model, feat), bf16),
            pltpu.VMEM((feat, model), bf16),
            pltpu.VMEM((3, total, feat), bf16),
            pltpu.VMEM((2 * rows, feat), bf16),
            pltpu.VMEM((rows, model), bf16),
            pltpu.VMEM((2, h, rows, model), bf16),
            pltpu.VMEM((3, rows, feat), jnp.float32),
            pltpu.VMEM((3, 1, feat), jnp.float32),
            dma((2, h, 2)),
            dma((2, h, 2)),
            dma((2, PIECES)),
            dma((2, PIECES)),
            dma((2, h + 1, CHUNKS)),
            dma((2, h + 1, CHUNKS)),
            dma,
            dma((3,)),
            dma,
            dma((2, slots)),
            dma((2, slots)),
        ],
        compiler_params=pltpu.CompilerParams(
            collective_id=0, has_side_effects=True, vmem_limit_bytes=67_043_328
        ),
        name="attention_sublayer",
    )(tokens, ln_gain[None, :], ln_bias[None, :], jnp.transpose(w_qkv, (1, 0, 2)), b_qkv, w_out,
      b_out[None, :], kv_cache, page_table, lengths)


def solution(mesh):
    placed = (
        P(("dp", "tp"), None),
        P(),
        P(),
        P(None, None, "tp"),
        P(None, "tp"),
        P("tp", None),
        P(),
        P(None, "dp", None, "tp"),
        P("dp", None),
        P("dp"),
    )
    return jax.shard_map(
        functools.partial(body, ring_order(mesh)),
        mesh=mesh,
        in_specs=placed,
        out_specs=(P(("dp", "tp"), None), P(None, "dp", None, "tp")),
        check_vma=False,
    )
```

```python
import functools
import math

import jax
import jax.numpy as jnp
import numpy as np
from jax import lax
from jax.experimental import pallas as pl
from jax.experimental.pallas import tpu as pltpu
from jax.sharding import PartitionSpec as P

HD = 128
CHUNKS = 4
PIECES = 4
MESH = pl.DeviceIdType.MESH

norm_eps = 1e-05


def ring_order(mesh):
    n = mesh.shape["tp"]
    line = np.moveaxis(mesh.devices, mesh.axis_names.index("tp"), -1).reshape(-1, n)[0]
    coords = [tuple(getattr(d, "coords", None) or ()) for d in line]
    wide = len({c[0] for c in coords if c})
    if wide < 2 or n % wide or (n // wide) % 2:
        return list(range(n))
    tall = n // wide
    order = [0]
    for z in range(tall):
        xs = range(1, wide) if z % 2 == 0 else range(wide - 1, 0, -1)
        order += [z * wide + x for x in xs]
    order += [z * wide for z in range(tall - 1, 0, -1)]
    return order


def pick(table, index):
    value = jnp.int32(0)
    for k, entry in enumerate(table):
        value = value + jnp.where(index == k, entry, 0)
    return value


def fused(order, x_hbm, gain_ref, shift_ref, w_hbm, b_ref, wo_hbm, bo_ref, cache_hbm, table_ref,
          len_ref, out_ref, kv_hbm,
          xg, w_v, wo_v, proj, att, first, rs, held, bias,
          ag_send, ag_recv, tail_send, tail_recv, rs_send, rs_recv,
          x_sem, w_sem, wo_sem, in_sem, kv_sem):
    n = len(order)
    h = n // 2
    rows, model = x_hbm.shape
    mid = model // 2
    feat = w_v.shape[2]
    total = proj.shape[1]
    me = lax.axis_index("tp")
    inverse = [order.index(i) for i in range(n)]
    place = pick(inverse, me)

    def at(offset):
        return pick(order, lax.rem(place + offset + n, n))

    peers = (at(1), at(-1))
    x_copy = pltpu.make_async_copy(x_hbm, first, x_sem)
    x_copy.start()
    barrier = pltpu.get_barrier_semaphore()
    for peer in peers:
        pl.semaphore_signal(barrier, inc=1, device_id={"tp": peer}, device_id_type=MESH)
    x_copy.wait()
    for c in range(3):
        pltpu.make_async_copy(w_hbm.at[c], w_v.at[c], w_sem.at[c]).start()
    wo_copy = pltpu.make_async_copy(wo_hbm, wo_v, wo_sem)
    wo_copy.start()

    for c in range(3):
        bias[c] = b_ref[pl.ds(c, 1), :]
    group = math.gcd(rows, 16)

    @pl.loop(0, rows // group)
    def _(i):
        part = pl.ds(pl.multiple_of(i * group, group), group)
        floats = first[part, :].astype(jnp.float32)
        center = jnp.mean(floats, axis=-1, keepdims=True)
        spread = jnp.mean(jnp.square(floats - center), axis=-1, keepdims=True)
        normed = ((floats - center) * lax.rsqrt(spread + norm_eps) * gain_ref[...]
                  + shift_ref[...]).astype(jnp.bfloat16)
        xg[0, part, :] = normed[:, :mid]
        xg[1, part, :] = normed[:, mid:]

    pl.semaphore_wait(barrier, 2)

    def slot(way, s):
        return 0 if s == 0 else n - 1 if s == h else 2 * s - 1 + way

    def gather(way, s, half):
        return pltpu.make_async_remote_copy(
            src_ref=xg.at[half, pl.ds(slot(way, s - 1) * rows, rows)],
            dst_ref=xg.at[half, pl.ds(slot(way, s) * rows, rows)],
            send_sem=ag_send.at[way, s, half], recv_sem=ag_recv.at[way, s, half],
            device_id={"tp": peers[way]}, device_id_type=MESH)

    piece = mid // PIECES

    def tail(way, e):
        cols = pl.ds(e * piece, piece)
        return pltpu.make_async_remote_copy(
            src_ref=xg.at[way, pl.ds(slot(way, h - 1) * rows, rows), cols],
            dst_ref=xg.at[way, pl.ds((n - 1) * rows, rows), cols],
            send_sem=tail_send.at[way, e], recv_sem=tail_recv.at[way, e],
            device_id={"tp": peers[way]}, device_id_type=MESH)

    gathers = [(way, s, k if way == 0 else 1 - k)
               for s in range(1, h) for k in range(2) for way in range(2)]
    for g in gathers:
        if g[1] == 1:
            gather(*g).start()
    for c in range(3):
        pltpu.make_async_copy(w_hbm.at[c], w_v.at[c], w_sem.at[c]).wait()

    tn = math.gcd(feat, 768)

    def project(lhs, owners):
        @pl.loop(0, 3)
        def _(c):
            @pl.loop(0, feat // tn)
            def _(j):
                cols = pl.ds(pl.multiple_of(j * tn, tn), tn)
                acc = jnp.dot(lhs(0), w_v[c, pl.ds(0, mid), cols],
                              preferred_element_type=jnp.float32)
                acc += jnp.dot(lhs(1), w_v[c, pl.ds(mid, mid), cols],
                               preferred_element_type=jnp.float32)
                done = (acc + bias[c, :, cols]).astype(jnp.bfloat16)
                for i, owner in enumerate(owners):
                    dst = pl.ds(pl.multiple_of(owner * rows, rows), rows)
                    proj[c, dst, cols] = done[i * rows:(i + 1) * rows]

    def project_tail(e):
        far = pl.ds((n - 3) * rows, 3 * rows)
        owners = [at(1 - h), at(h - 1), at(h)]
        here = pl.ds(e * piece, piece)

        @pl.loop(0, 3)
        def _(c):
            @pl.loop(0, feat // tn)
            def _(j):
                cols = pl.ds(pl.multiple_of(j * tn, tn), tn)
                acc = jnp.dot(xg[0, far, here], w_v[c, here, cols],
                              preferred_element_type=jnp.float32)
                acc += jnp.dot(xg[1, far, here], w_v[c, pl.ds(mid + e * piece, piece), cols],
                               preferred_element_type=jnp.float32)
                if e > 0:
                    acc += held[c, :, cols]
                if e < PIECES - 1:
                    held[c, :, cols] = acc
                else:
                    done = (acc + bias[c, :, cols]).astype(jnp.bfloat16)
                    for i, owner in enumerate(owners):
                        dst = pl.ds(pl.multiple_of(owner * rows, rows), rows)
                        proj[c, dst, cols] = done[i * rows:(i + 1) * rows]

    project(lambda half: xg[half, pl.ds(0, rows)], [me])
    for s in range(1, h):
        for g in gathers:
            if g[1] == s:
                way, _, half = g
                gather(*g).wait_recv()
                if s + 1 < h:
                    gather(way, s + 1, half).start()
                elif half == way:
                    for e in range(PIECES):
                        tail(way, e).start()
        if s < h - 1:
            project(lambda half: xg[half, pl.ds((2 * s - 1) * rows, 2 * rows)], [at(-s), at(s)])
    for e in range(PIECES):
        for way in range(2):
            tail(way, e).wait_recv()
        project_tail(e)

    slots, page_len = cache_hbm.shape[1:3]

    def page(i, s):
        return w_v.at[i, pl.ds(s * page_len, page_len)]

    def cache_in(i, s):
        return pltpu.make_async_copy(cache_hbm.at[i, s], page(i, s), in_sem.at[i, s])

    def cache_out(i, s):
        return pltpu.make_async_copy(page(i, s), kv_hbm.at[i, s], kv_sem.at[i, s])

    pages = [(i, s) for i in range(2) for s in range(slots)]
    length = len_ref[0]

    def fill_pages():
        for i, s in pages:
            cache_in(i, s).wait()
        pos = lax.broadcasted_iota(jnp.int32, (page_len, feat), 0)

        @pl.loop(0, slots)
        def _(s):
            here = pl.ds(pl.multiple_of(s * page_len, page_len), page_len)
            for i in range(2):
                held_page = w_v[i, here, :]
                for k in range(table_ref.shape[1]):
                    left = jnp.where(table_ref[0, k] == s, length - k * page_len, 0)
                    held_page = jnp.where(
                        pos < left, proj[i + 1, pl.ds(k * page_len, page_len), :], held_page)
                w_v[i, here, :] = held_page

        for i, s in pages:
            cache_out(i, s).start()

    scale = 1.0 / math.sqrt(HD)

    def attend(owners):
        key_pos = lax.broadcasted_iota(jnp.int32, (rows, total), 1)
        row_pos = lax.broadcasted_iota(jnp.int32, (rows, total), 0)

        heads = feat // HD
        per = 1 if len(owners) > 1 else math.gcd(heads, 3)

        @pl.loop(0, heads // per)
        def _(turn):
            for i, b in [(i, b) for i in range(per) for b in range(len(owners))]:
                owner = owners[b]
                cols = pl.ds(pl.multiple_of((turn * per + i) * HD, HD), HD)
                query = proj[0, pl.ds(pl.multiple_of(owner * rows, rows), rows), cols]
                scores = lax.dot_general(query, proj[1, :, cols], (((1,), (1,)), ((), ())),
                                         preferred_element_type=jnp.float32) * scale
                allowed = (key_pos <= row_pos + owner * rows) & (key_pos < length)
                scores = jnp.where(allowed, scores, -1e30)
                raised = jnp.exp(scores - jnp.max(scores, axis=-1, keepdims=True))
                share = 1.0 / jnp.sum(raised, axis=-1, keepdims=True)
                att[pl.ds(b * rows, rows), cols] = jnp.dot(
                    (raised * share).astype(jnp.bfloat16), proj[2, :, cols],
                    preferred_element_type=jnp.float32).astype(jnp.bfloat16)

    chunk = model // CHUNKS
    to = math.gcd(chunk, 768)

    def scatter(way, d, q):
        cols = pl.ds(q * chunk, chunk)
        src = first.at[:, cols] if d == h else rs.at[way, d, :, cols]
        return pltpu.make_async_remote_copy(
            src_ref=src, dst_ref=rs.at[way, d - 1, :, cols],
            send_sem=rs_send.at[way, d, q], recv_sem=rs_recv.at[way, d, q],
            device_id={"tp": peers[way]}, device_id_type=MESH)

    scatters = [(way, d, q) for d in range(h, 0, -1) for q in range(CHUNKS) for way in range(2)
                if d < h or way == q // (CHUNKS // 2)]

    wo_copy.wait()
    attend([at(h)])
    half = CHUNKS // 2
    turns = [0, half] + [c for c in range(CHUNKS) if c not in (0, half)]
    for q in turns:
        @pl.loop(0, chunk // to)
        def _(j):
            cols = pl.ds(pl.multiple_of(q * chunk + j * to, to), to)
            first[:, cols] = jnp.dot(att[pl.ds(0, rows), :], wo_v[:, cols],
                                     preferred_element_type=jnp.float32).astype(jnp.bfloat16)
        for way in range(2):
            if (way, h, q) in scatters:
                scatter(way, h, q).start()

    for i, s in pages:
        cache_in(i, s).start()

    for d in range(h - 1, 0, -1):
        attend([at(d), at(-d)])
        for q in turns:
            have = [(way, d + 1, q) in scatters for way in range(2)]
            for way in range(2):
                if have[way]:
                    scatter(way, d + 1, q).wait_recv()

            @pl.loop(0, chunk // to)
            def _(j):
                cols = pl.ds(pl.multiple_of(q * chunk + j * to, to), to)
                part = jnp.dot(att[...], wo_v[:, cols], preferred_element_type=jnp.float32)
                for way in range(2):
                    mine = part[way * rows:(way + 1) * rows]
                    if have[way]:
                        mine = mine + rs[way, d, :, cols].astype(jnp.float32)
                    rs[way, d, :, cols] = mine.astype(jnp.bfloat16)
            for way in range(2):
                scatter(way, d, q).start()
        if d == h - 1:
            fill_pages()

    attend([me])
    for q in turns:
        for way in range(2):
            scatter(way, 1, q).wait_recv()

        @pl.loop(0, chunk // to)
        def _(j):
            cols = pl.ds(pl.multiple_of(q * chunk + j * to, to), to)
            part = jnp.dot(att[pl.ds(0, rows), :], wo_v[:, cols],
                           preferred_element_type=jnp.float32)
            part += rs[0, 0, :, cols].astype(jnp.float32) + rs[1, 0, :, cols].astype(jnp.float32)
            out_ref[:, cols] = (part + bo_ref[:, cols]).astype(jnp.bfloat16)

    for g in gathers:
        gather(*g).wait_send()
    for e in range(PIECES):
        for way in range(2):
            tail(way, e).wait_send()
    for g in scatters:
        scatter(*g).wait_send()
    for i, s in pages:
        cache_out(i, s).wait()


def body(order, tokens, ln_gain, ln_bias, w_qkv, b_qkv, w_out, b_out, kv_cache, page_table,
         lengths):
    n = len(order)
    h = n // 2
    rows, model = tokens.shape
    feat = w_qkv.shape[2]
    total = rows * n
    vmem = pl.BlockSpec(memory_space=pltpu.VMEM)
    anywhere = pl.BlockSpec(memory_space=pl.ANY)
    bf16 = jnp.bfloat16
    smem = pl.BlockSpec(memory_space=pltpu.SMEM)
    slots = kv_cache.shape[1]
    dma = pltpu.SemaphoreType.DMA
    return pl.pallas_call(
        functools.partial(fused, order),
        out_shape=(
            jax.ShapeDtypeStruct((rows, model), bf16),
            jax.ShapeDtypeStruct(kv_cache.shape, bf16),
        ),
        in_specs=[anywhere, vmem, vmem, anywhere, vmem, anywhere, vmem, anywhere, smem, smem],
        out_specs=(vmem, anywhere),
        scratch_shapes=[
            pltpu.VMEM((2, total, model // 2), bf16),
            pltpu.VMEM((3, model, feat), bf16),
            pltpu.VMEM((feat, model), bf16),
            pltpu.VMEM((3, total, feat), bf16),
            pltpu.VMEM((2 * rows, feat), bf16),
            pltpu.VMEM((rows, model), bf16),
            pltpu.VMEM((2, h, rows, model), bf16),
            pltpu.VMEM((3, 3 * rows, feat), jnp.float32),
            pltpu.VMEM((3, 1, feat), jnp.float32),
            dma((2, h, 2)),
            dma((2, h, 2)),
            dma((2, PIECES)),
            dma((2, PIECES)),
            dma((2, h + 1, CHUNKS)),
            dma((2, h + 1, CHUNKS)),
            dma,
            dma((3,)),
            dma,
            dma((2, slots)),
            dma((2, slots)),
        ],
        compiler_params=pltpu.CompilerParams(
            collective_id=0, has_side_effects=True, vmem_limit_bytes=67_043_328
        ),
        name="attention_sublayer",
    )(tokens, ln_gain[None, :], ln_bias[None, :], jnp.transpose(w_qkv, (1, 0, 2)), b_qkv, w_out,
      b_out[None, :], kv_cache, page_table, lengths)


def solution(mesh):
    placed = (
        P(("dp", "tp"), None),
        P(),
        P(),
        P(None, None, "tp"),
        P(None, "tp"),
        P("tp", None),
        P(),
        P(None, "dp", None, "tp"),
        P("dp", None),
        P("dp"),
    )
    return jax.shard_map(
        functools.partial(body, ring_order(mesh)),
        mesh=mesh,
        in_specs=placed,
        out_specs=(P(("dp", "tp"), None), P(None, "dp", None, "tp")),
        check_vma=False,
    )
```
